256 devices in a mesh: grp: 8 (over y, core), shard: 32 (over x, z).
Axes of the slice: x: 4, y: 4, z: 8, core: 2. Of those that a mesh axis runs over, the one named last changes fastest.
Arguments:
- grads: float32 [8, 32, 3456, 512], P('grp', 'shard'), may hold values from -6 to 6
- master: float32 [3456, 512], P('shard'), may hold values from -0.109375 to 0.109375
- moment_one: float32 [3456, 512], P('shard'), may hold values from -0.0004510549 to 0.0004510549
- moment_two: float32 [3456, 512], P('shard'), may hold values from 1.13028066e-10 to 2.8257017e-09
- step_count: int32 [1], replicated, may hold values from 1 to 59
Outputs:
- new_master: float32 [3456, 512], P('shard')
- new_moment_one: float32 [3456, 512], P('shard')
- new_moment_two: float32 [3456, 512], P('shard')
- weights: bfloat16 [3456, 512], replicated
The draws below stay inside these ranges and needn't reach their ends.
All inputs are finite; a program needn't handle non-finite values.
Results may differ from the reference program's by a relative error of at most 0.0004.
Values may be sent and summed in bfloat16 or wider, within the bound.
No kernel may reach another device: no remote copies, remote signals or barrier semaphores. Data moves between devices by JAX's collectives and lax.ppermute only.
A program may use at most 128 MiB of HBM per device.

```python
import math
import jax
import jax.numpy as jnp
from jax import lax

IN = 3456
RANK = 512
N_GRP = 8
N_SHARD = 32


def strengthened(drawn, key, source, target, shards_of, factor):
    owner, partner = [(jnp.arange(drawn.shape[dim]) // (drawn.shape[dim] // shards_of)).reshape([-1 if axis == dim else 1 for axis in range(drawn.ndim)]) for dim in (source, target)]
    chosen = jax.random.permutation(key, shards_of)[partner]
    strong = (owner == chosen) | (owner == (partner + shards_of // 2) % shards_of)
    return jnp.where(strong, factor * drawn, drawn)


def shard_levels(key, dims, cuts, least, largest):
    loudness, own = 1.0, jax.random.fold_in(key, 6)
    for position, parts in cuts:
        steps = jnp.exp(jax.random.uniform(jax.random.fold_in(own, position), (parts,), jnp.float32, least / len(cuts), largest / len(cuts)))
        loudness = loudness * jnp.repeat(steps, dims[position] // parts).reshape([-1 if axis == position else 1 for axis in range(len(dims))])
    return loudness


def bell_draw(key, dims, deviation, reach, split=(), kind=jnp.bfloat16):
    result = deviation * jax.random.normal(key, dims, jnp.float32)
    if split:
        result = result * shard_levels(key, dims, split, -0.22, 0.18)
    return jnp.clip(result, -reach, reach).astype(kind)


def heavy_noise(rng, extent, deviation, reach, cuts, heavy, held_as=jnp.bfloat16):
    drawn = deviation * jax.random.normal(rng, extent, jnp.float32)
    if cuts:
        drawn = drawn * shard_levels(rng, extent, cuts, -0.22, 0.18)
    return jnp.clip(strengthened(drawn, jax.random.fold_in(rng, 3), *heavy), -reach, reach).astype(held_as)


def setup_inputs(seed: int = 0) -> dict:
    keys = jax.random.split(jax.random.key(seed), 6)
    grads = heavy_noise(keys[0], (N_GRP, N_SHARD, IN, RANK), 1.0, 6.0, ((0, 8), (1, 32)), (1, 2, 32, 2.75), jnp.float32)
    master = bell_draw(keys[1], (IN, RANK), IN ** -0.5, 0.109375, ((0, 32),), jnp.float32)
    moment_one = bell_draw(keys[2], (IN, RANK), (0.1 * (IN * RANK) ** -0.5), 0.0004510549, ((0, 32),), jnp.float32)
    moment_two = jnp.clip(jnp.exp(math.log(2.8257016726485062e-09) - 3.218876 * jax.random.uniform(keys[3], (IN, RANK), jnp.float32) ** shard_levels(keys[3], (IN, RANK), ((0, 32),), -0.2, 0.2)), 1.1302806607327298e-10, 2.8257016726485062e-09)
    step_count = jax.random.randint(keys[4], (1,), 1, 60).astype(jnp.int32)
    return dict(grads=grads, master=master, moment_one=moment_one, moment_two=moment_two, step_count=step_count)


def reference(grads, master, moment_one, moment_two, step_count):
    summed = lax.optimization_barrier(jnp.sum(grads, axis=(0, 1), dtype=jnp.float32))
    norm = jnp.sqrt(jnp.sum(summed * summed))
    clip = jnp.minimum(jnp.float32(1.0), 1.0 / (norm + 1e-06))
    gradient = clip * summed
    new_one = 0.9 * moment_one + 0.1 * gradient
    new_two = 0.999 * moment_two + 0.001 * gradient * gradient
    steps = step_count[0].astype(jnp.float32)
    first_fix = 1.0 - jnp.power(jnp.float32(0.9), steps)
    second_fix = 1.0 - jnp.power(jnp.float32(0.999), steps)
    update = new_one / first_fix / (jnp.sqrt(new_two / second_fix) + 1e-08)
    new_master = master - 0.01 * (update + 0.01 * master)
    return (new_master, new_one, new_two, new_master.astype(jnp.bfloat16))
```

```python
import jax
import jax.numpy as jnp
from jax import lax
from jax.experimental import pallas as pl
from jax.experimental.pallas import tpu as pltpu
from jax.sharding import Mesh
from jax.sharding import PartitionSpec as P

GRP = ("y", "c")
SHARD = ("x", "zp", "zl")
PLANE = ("x", "y")
PAIR = ("y", "c", "zl")
PAIRS = ("x", "zp")

STARTS = (0, 56, 112, 160)
PART = 56
HALF_STARTS = (0, 104)
HALF = 112


def add_halves_kernel(c_ref, mine_ref, theirs_ref, out_ref):
    for zp in range(4):
        for zl in range(2):
            for y in range(4):
                rows = pl.ds(zp * 216 + STARTS[y], PART)
                cols = pl.ds(zl * 128, 128)
                out_ref[0, y, pl.ds((zp * 2 + zl) * PART, PART), :] = mine_ref[rows, cols] + theirs_ref[rows, cols]


def add_halves(c, local, theirs):
    return pl.pallas_call(
        add_halves_kernel,
        grid_spec=pltpu.PrefetchScalarGridSpec(
            num_scalar_prefetch=1,
            grid=(4,),
            in_specs=[
                pl.BlockSpec((864, 256), lambda i, c: (i, c[0])),
                pl.BlockSpec((864, 256), lambda i, c: (i, 0)),
            ],
            out_specs=pl.BlockSpec((1, 4, 8 * PART, 128), lambda i, c: (i, 0, 0, 0)),
        ),
        out_shape=jax.ShapeDtypeStruct((4, 4, 8 * PART, 128), jnp.float32),
    )(c, local, theirs)


def place_pair(buf, parts_ref):
    for y in range(4):
        for tc in range(4):
            buf[pl.ds(STARTS[y], PART), pl.ds(tc * 128, 128)] = parts_ref[y * 4 + tc]


def squares_kernel(parts_ref, sum_ref, total_ref):
    place_pair(sum_ref, parts_ref)
    total = jnp.zeros((8, 512), jnp.float32)
    for t in range(27):
        row = sum_ref[pl.ds(t * 8, 8), :]
        total = total + row * row
    total = jnp.sum(total)
    total_ref[...] = jnp.full(total_ref.shape, total, jnp.float32)


def squares(parts):
    return pl.pallas_call(
        squares_kernel,
        out_shape=(
            jax.ShapeDtypeStruct((216, 512), jnp.float32),
            jax.ShapeDtypeStruct((16, 1, 128), jnp.float32),
        ),
    )(parts)


def adam_kernel(where_ref, fixes_ref, summed_ref, totals_ref, *refs):
    (w_own, w_other, a_own, a_other, b_own, b_other, w_out, a_out, b_out, send_ref, w, a, b) = refs
    y, c, zl = where_ref[0], where_ref[1], where_ref[2]
    first = zl == 0
    for buf, own, other in ((w, w_own, w_other), (a, a_own, a_other), (b, b_own, b_other)):
        buf[pl.ds(0, 108), :] = jnp.where(first, own[...], other[...])
        buf[pl.ds(108, 108), :] = jnp.where(first, other[...], own[...])
    total = jnp.sum(totals_ref[...], axis=0)
    norm = jnp.sqrt(total)
    clip = jnp.minimum(jnp.float32(1.0), 1.0 / (norm + 1e-06))
    clip = clip[:, :1]
    gradient = clip * summed_ref[...]
    new_one = 0.9 * a[...] + 0.1 * gradient
    new_two = 0.999 * b[...] + 0.001 * gradient * gradient
    update = new_one / fixes_ref[0] / (jnp.sqrt(new_two / fixes_ref[1]) + 1e-08)
    new_master = w[...] - 0.01 * (update + 0.01 * w[...])
    a[...] = new_one
    b[...] = new_two
    w[...] = new_master
    for buf, out in ((w, w_out), (a, a_out), (b, b_out)):
        out[...] = jnp.where(first, buf[pl.ds(0, 108), :], buf[pl.ds(108, 108), :])
    low = w[pl.ds(0, HALF), pl.ds(pl.multiple_of(y * 128, 128), 128)]
    high = w[pl.ds(HALF_STARTS[1], HALF), pl.ds(pl.multiple_of(y * 128, 128), 128)]
    part = jnp.where(c == 0, low, high).astype(jnp.bfloat16)
    for k in range(4):
        send_ref[k] = part


def adam(where, fixes, summed, totals, states):
    smem = pl.BlockSpec(memory_space=pltpu.SMEM)
    vmem = pl.BlockSpec(memory_space=pltpu.VMEM)
    rows = jax.ShapeDtypeStruct((108, 512), jnp.float32)
    return pl.pallas_call(
        adam_kernel,
        in_specs=[smem, smem] + [vmem] * 8,
        out_shape=(rows, rows, rows, jax.ShapeDtypeStruct((4, HALF, 128), jnp.bfloat16)),
        scratch_shapes=[pltpu.VMEM((216, 512), jnp.float32)] * 3,
    )(where, fixes, summed, totals, *states)


def assemble_kernel(c_ref, mine_ref, theirs_ref, out_ref):
    first = c_ref[0] == 0
    for zp in range(4):
        for y in range(4):
            for half in range(2):
                rows = pl.ds(zp * 216 + HALF_STARTS[half], HALF)
                mine, theirs = mine_ref[0, y, zp], theirs_ref[0, y, zp]
                value = jnp.where(first == (half == 0), mine, theirs)
                out_ref[rows, pl.ds(y * 128, 128)] = value


def assemble(c, mine, theirs):
    block = pl.BlockSpec((1, 4, 4, HALF, 128), lambda i, c: (i, 0, 0, 0, 0))
    return pl.pallas_call(
        assemble_kernel,
        grid_spec=pltpu.PrefetchScalarGridSpec(
            num_scalar_prefetch=1,
            grid=(4,),
            in_specs=[block, block],
            out_specs=pl.BlockSpec((864, 512), lambda i, c: (i, 0)),
        ),
        out_shape=jax.ShapeDtypeStruct((3456, 512), jnp.bfloat16),
    )(c, mine, theirs)


def exchanged(value, axes):
    return lax.all_to_all(value, axes, split_axis=0, concat_axis=0, tiled=True)


def swapped(value, axis):
    return lax.ppermute(value, axis, [(0, 1), (1, 0)])


def shards(grads, master, moment_one, moment_two, step_count):
    y, c, zl = (lax.axis_index(axis) for axis in PAIR)
    where = jnp.stack([y, c, zl]).astype(jnp.int32)
    side = where[1:2]
    local = grads[0, 0]
    theirs = swapped(lax.dynamic_slice(local, (0, 256 * (1 - c)), (3456, 256)), "c")
    states = []
    for own in (master, moment_one, moment_two):
        states += [own, swapped(own, "zl")]
    chunks = add_halves(side, local, theirs).reshape(16, 8 * PART, 128)
    columns = exchanged(chunks, PLANE).sum(axis=0)
    part = exchanged(columns.reshape(8, PART, 128), ("zp", "zl")).sum(axis=0)
    parts = exchanged(jnp.broadcast_to(part, (16, PART, 128)), PAIR)
    summed, total = squares(parts)
    totals = exchanged(total, PAIRS)
    steps = step_count[0].astype(jnp.float32)
    first_fix = 1.0 - jnp.power(jnp.float32(0.9), steps)
    second_fix = 1.0 - jnp.power(jnp.float32(0.999), steps)
    new_master, new_one, new_two, sent = adam(where, jnp.stack([first_fix, second_fix]), summed, totals, states)
    column = exchanged(sent, "zp")
    mine = exchanged(jnp.broadcast_to(column, (16, *column.shape)), PLANE)
    other = swapped(mine, "c")
    grouped = (4, 4, 4, HALF, 128)
    weights = assemble(side, mine.reshape(grouped), other.reshape(grouped))
    return (new_master, new_one, new_two, weights)


def solution(mesh):
    finer = Mesh(mesh.devices.reshape(4, 2, 4, 4, 2), ("y", "c", "x", "zp", "zl"))
    in_specs = (P(GRP, SHARD, None, None), P(SHARD, None), P(SHARD, None), P(SHARD, None), P())
    out_specs = (P(SHARD, None), P(SHARD, None), P(SHARD, None), P())
    return jax.shard_map(
        shards, mesh=finer, in_specs=in_specs, out_specs=out_specs, check_vma=False
    )
```

```python
import jax
import jax.numpy as jnp
from jax import lax
from jax.experimental import pallas as pl
from jax.experimental.pallas import tpu as pltpu
from jax.sharding import Mesh
from jax.sharding import PartitionSpec as P

GRP = ("y", "c")
SHARD = ("x", "zp", "zl")
PLANE = ("x", "y")
PAIR = ("y", "c", "zl")
PAIRS = ("x", "zp")

STARTS = (0, 56, 112, 160)
PART = 56
COLUMN = 8 * PART
HALF_STARTS = (0, 104)
HALF = 112
LIMIT = pltpu.CompilerParams(vmem_limit_bytes=24 * 2**20)


def add_halves_kernel(c_ref, mine_ref, theirs_ref, out_ref, sums):
    base = pl.program_id(0) * 864
    for y in range(4):
        peak = jnp.zeros((8, 128), jnp.float32)
        for z in range(8):
            start = (z // 2) * 216 + STARTS[y]
            cols = pl.ds((z % 2) * 128, 128)
            for t in range(0, PART, 8):
                rows = pl.ds(start + t, 8)
                value = mine_ref[rows, cols] + theirs_ref[pl.ds(base + start + t, 8), cols]
                peak = jnp.maximum(peak, jnp.abs(value))
                sums[pl.ds(z * PART + t, 8), :] = value
        peak = jnp.max(peak, axis=0, keepdims=True)
        level = jnp.maximum(jnp.ceil(4.0 * jnp.log2(peak) + 0.02), -400.0)
        inverse = 32767.0 * jnp.exp2(-0.25 * level)
        for t in range(0, COLUMN, PART):
            scaled = jnp.round(sums[pl.ds(t, PART), :] * inverse)
            out_ref[0, y, pl.ds(t, PART), :] = scaled.astype(jnp.int32).astype(jnp.int16)
        level = jnp.broadcast_to(level, (8, 128))
        out_ref[0, y, pl.ds(COLUMN, 8), :] = level.astype(jnp.int32).astype(jnp.int16)


def add_halves(c, local, theirs):
    return pl.pallas_call(
        add_halves_kernel,
        compiler_params=LIMIT,
        grid_spec=pltpu.PrefetchScalarGridSpec(
            num_scalar_prefetch=1,
            grid=(4,),
            in_specs=[
                pl.BlockSpec((864, 256), lambda i, c: (i, c[0])),
                pl.BlockSpec(memory_space=pltpu.VMEM),
            ],
            out_specs=pl.BlockSpec((1, 4, COLUMN + 8, 128), lambda i, c: (i, 0, 0, 0)),
            scratch_shapes=[pltpu.VMEM((COLUMN, 128), jnp.float32)],
        ),
        out_shape=jax.ShapeDtypeStruct((4, 4, COLUMN + 8, 128), jnp.int16),
    )(c, local, in_vmem(theirs))


def sum_plane_kernel(coded_ref, out_ref):
    scales = []
    for k in range(16):
        level = coded_ref[k, pl.ds(COLUMN, 8), :].astype(jnp.int32).astype(jnp.float32)
        scales.append(jnp.exp2(0.25 * level) * (1.0 / 32767.0))
    for z in range(8):
        rows = pl.ds(z * PART, PART)
        total = jnp.zeros((PART // 8, 8, 128), jnp.float32)
        for k in range(16):
            value = coded_ref[k, rows, :].astype(jnp.int32).astype(jnp.float32)
            total = total + value.reshape(PART // 8, 8, 128) * scales[k]
        out_ref[z] = total.reshape(PART, 128)


def sum_plane(coded):
    return pl.pallas_call(
        sum_plane_kernel,
        compiler_params=LIMIT,
        in_specs=[pl.BlockSpec(memory_space=pltpu.VMEM)],
        out_specs=pl.BlockSpec(memory_space=pltpu.VMEM),
        out_shape=jax.ShapeDtypeStruct((8, PART, 128), jnp.float32),
    )(in_vmem(coded))


def place_pair(buf, parts_ref):
    for y in range(4):
        for tc in range(4):
            buf[pl.ds(STARTS[y], PART), pl.ds(tc * 128, 128)] = parts_ref[y * 4 + tc]


def squares_kernel(parts_ref, sum_ref, total_ref):
    place_pair(sum_ref, parts_ref)
    total = jnp.zeros((8, 512), jnp.float32)
    for t in range(27):
        row = sum_ref[pl.ds(t * 8, 8), :]
        total = total + row * row
    total = jnp.sum(total)
    total_ref[...] = jnp.full(total_ref.shape, total, jnp.float32)


def squares(parts):
    vmem = pl.BlockSpec(memory_space=pltpu.VMEM)
    return pl.pallas_call(
        squares_kernel,
        compiler_params=LIMIT,
        in_specs=[vmem],
        out_specs=(vmem, vmem),
        out_shape=(
            jax.ShapeDtypeStruct((216, 512), jnp.float32),
            jax.ShapeDtypeStruct((16, 8, 128), jnp.float32),
        ),
    )(in_vmem(parts))


def adam_kernel(where_ref, fixes_ref, summed_ref, totals_ref, *refs):
    (w_own, w_other, a_own, a_other, b_own, b_other, w_out, a_out, b_out, send_ref, w, a, b) = refs
    y, c, zl = where_ref[0], where_ref[1], where_ref[2]
    first = zl == 0
    for buf, own, other in ((w, w_own, w_other), (a, a_own, a_other), (b, b_own, b_other)):
        buf[pl.ds(0, 108), :] = jnp.where(first, own[...], other[...])
        buf[pl.ds(108, 108), :] = jnp.where(first, other[...], own[...])
    total = jnp.sum(totals_ref[...], axis=0)[:1]
    norm = jnp.sqrt(total)
    clip = jnp.minimum(jnp.float32(1.0), 1.0 / (norm + 1e-06))
    clip = clip[:, :1]
    gradient = clip * summed_ref[...]
    new_one = 0.9 * a[...] + 0.1 * gradient
    new_two = 0.999 * b[...] + 0.001 * gradient * gradient
    update = new_one / fixes_ref[0] / (jnp.sqrt(new_two / fixes_ref[1]) + 1e-08)
    new_master = w[...] - 0.01 * (update + 0.01 * w[...])
    a[...] = new_one
    b[...] = new_two
    w[...] = new_master
    for buf, out in ((w, w_out), (a, a_out), (b, b_out)):
        out[...] = jnp.where(first, buf[pl.ds(0, 108), :], buf[pl.ds(108, 108), :])
    low = w[pl.ds(0, HALF), pl.ds(pl.multiple_of(y * 128, 128), 128)]
    high = w[pl.ds(HALF_STARTS[1], HALF), pl.ds(pl.multiple_of(y * 128, 128), 128)]
    part = jnp.where(c == 0, low, high).astype(jnp.bfloat16)
    for k in range(4):
        send_ref[k] = part


def adam(where, fixes, summed, totals, states):
    smem = pl.BlockSpec(memory_space=pltpu.SMEM)
    vmem = pl.BlockSpec(memory_space=pltpu.VMEM)
    rows = jax.ShapeDtypeStruct((108, 512), jnp.float32)
    return pl.pallas_call(
        adam_kernel,
        compiler_params=LIMIT,
        in_specs=[smem, smem] + [vmem] * 8,
        out_shape=(rows, rows, rows, jax.ShapeDtypeStruct((4, HALF, 128), jnp.bfloat16)),
        scratch_shapes=[pltpu.VMEM((216, 512), jnp.float32)] * 3,
    )(where, fixes, in_vmem(summed), in_vmem(totals), *map(in_vmem, states))


def assemble_kernel(c_ref, mine_ref, theirs_ref, out_ref):
    x = pl.program_id(0)
    first = c_ref[0] == 0
    for zp in range(4):
        for y in range(4):
            mine, theirs = mine_ref[x * 4 + y, zp], theirs_ref[x * 4 + y, zp]
            cols = pl.ds(y * 128, 128)
            for half in range(2):
                rows = pl.ds(zp * 216 + HALF_STARTS[half], HALF)
                out_ref[rows, cols] = jnp.where(first == (half == 0), mine, theirs)


def assemble(c, mine, theirs):
    vmem = pl.BlockSpec(memory_space=pltpu.VMEM)
    return pl.pallas_call(
        assemble_kernel,
        compiler_params=LIMIT,
        grid_spec=pltpu.PrefetchScalarGridSpec(
            num_scalar_prefetch=1,
            grid=(4,),
            in_specs=[vmem, vmem],
            out_specs=pl.BlockSpec((864, 512), lambda i, c: (i, 0)),
        ),
        out_shape=jax.ShapeDtypeStruct((3456, 512), jnp.bfloat16),
    )(c, in_vmem(mine), in_vmem(theirs))


def in_vmem(value):
    return pltpu.with_memory_space_constraint(value, pltpu.VMEM)


def exchanged(value, axes):
    return lax.all_to_all(value, axes, split_axis=0, concat_axis=0, tiled=True)


def swapped(value, axis):
    return lax.ppermute(value, axis, [(0, 1), (1, 0)])


def shards(grads, master, moment_one, moment_two, step_count):
    y, c, zl = (lax.axis_index(axis) for axis in PAIR)
    where = jnp.stack([y, c, zl]).astype(jnp.int32)
    side = where[1:2]
    local = grads[0, 0]
    theirs = swapped(lax.dynamic_slice(local, (0, 256 * (1 - c)), (3456, 256)), "c")
    states = []
    for own in (master, moment_one, moment_two):
        states += [own, swapped(own, "zl")]
    coded = exchanged(add_halves(side, local, theirs).reshape(16, COLUMN + 8, 128), PLANE)
    coded, states = lax.optimization_barrier((coded, states))
    part = exchanged(sum_plane(coded), ("zp", "zl")).sum(axis=0)
    parts = exchanged(jnp.broadcast_to(part, (16, PART, 128)), PAIR)
    summed, total = squares(parts)
    totals = exchanged(total, PAIRS)
    steps = step_count[0].astype(jnp.float32)
    first_fix = 1.0 - jnp.power(jnp.float32(0.9), steps)
    second_fix = 1.0 - jnp.power(jnp.float32(0.999), steps)
    new_master, new_one, new_two, sent = adam(where, jnp.stack([first_fix, second_fix]), summed, totals, states)
    column = exchanged(sent, "zp")
    mine = exchanged(jnp.broadcast_to(column, (16, *column.shape)), PLANE)
    other = swapped(mine, "c")
    weights = assemble(side, mine, other)
    return (new_master, new_one, new_two, weights)


def solution(mesh):
    finer = Mesh(mesh.devices.reshape(4, 2, 4, 4, 2), ("y", "c", "x", "zp", "zl"))
    in_specs = (P(GRP, SHARD, None, None), P(SHARD, None), P(SHARD, None), P(SHARD, None), P())
    out_specs = (P(SHARD, None), P(SHARD, None), P(SHARD, None), P())
    return jax.shard_map(
        shards, mesh=finer, in_specs=in_specs, out_specs=out_specs, check_vma=False
    )
```

```python
import jax
import jax.numpy as jnp
from jax import lax
from jax.experimental import pallas as pl
from jax.experimental.pallas import tpu as pltpu
from jax.sharding import Mesh
from jax.sharding import PartitionSpec as P

GRP = ("y", "c")
SHARD = ("x", "z")
PLANE = ("x", "y")

PART = 56
STARTS = (0, 52)
SHARED = 4
CUTS = ((0, PART),)
LIMIT = pltpu.CompilerParams(vmem_limit_bytes=24 * 2**20)
VMEM = pl.BlockSpec(memory_space=pltpu.VMEM)
SMEM = pl.BlockSpec(memory_space=pltpu.SMEM)


def in_vmem(value):
    return pltpu.with_memory_space_constraint(value, pltpu.VMEM)


def exchanged(value, axes):
    return lax.all_to_all(value, axes, split_axis=0, concat_axis=0, tiled=True)


def swapped(value, axis):
    return lax.ppermute(value, axis, [(0, 1), (1, 0)])


def rotated(value, axis):
    n = lax.axis_size(axis)
    return [value] + [lax.ppermute(value, axis, [(i, (i + k) % n) for i in range(n)]) for k in range(1, n)]


def code_sums(c, local, theirs, cut):
    first, length = cut
    column = 8 * length

    def kernel(c_ref, mine_ref, theirs_ref, out_ref, sums):
        for y in range(4):
            cols = pl.ds((y // 2) * 128, 128)
            peak = jnp.zeros((8, 128), jnp.float32)
            for z in range(8):
                start = 108 * z + STARTS[y % 2] + first
                for t in range(0, length, 8):
                    rows = pl.ds(start + t, 8)
                    value = mine_ref[rows, cols] + theirs_ref[rows, cols]
                    peak = jnp.maximum(peak, jnp.abs(value))
                    sums[pl.ds(z * length + t, 8), :] = value
            peak = jnp.max(peak, axis=0, keepdims=True)
            level = jnp.maximum(jnp.ceil(4.0 * jnp.log2(peak) + 0.02), -400.0)
            inverse = 32767.0 * jnp.exp2(-0.25 * level)
            for t in range(0, column, length):
                scaled = jnp.round(sums[pl.ds(t, length), :] * inverse)
                out_ref[0, y, pl.ds(t, length), :] = scaled.astype(jnp.int32).astype(jnp.int16)
            level = jnp.broadcast_to(level, (8, 128))
            out_ref[0, y, pl.ds(column, 8), :] = level.astype(jnp.int32).astype(jnp.int16)

    coded = pl.pallas_call(
        kernel,
        compiler_params=LIMIT,
        grid_spec=pltpu.PrefetchScalarGridSpec(
            num_scalar_prefetch=1,
            grid=(4,),
            in_specs=[
                pl.BlockSpec((864, 256), lambda i, c: (i, c[0])),
                pl.BlockSpec((864, 256), lambda i, c: (i, 0)),
            ],
            out_specs=pl.BlockSpec((1, 4, column + 8, 128), lambda i, c: (i, 0, 0, 0)),
            scratch_shapes=[pltpu.VMEM((column, 128), jnp.float32)],
        ),
        out_shape=jax.ShapeDtypeStruct((4, 4, column + 8, 128), jnp.int16),
    )(c, local, in_vmem(theirs))
    return coded.reshape(16, column + 8, 128)


def sum_coded(coded, cut):
    length = cut[1]
    column = 8 * length

    def kernel(coded_ref, out_ref):
        scales = []
        for k in range(16):
            level = coded_ref[k, pl.ds(column, 8), :].astype(jnp.int32).astype(jnp.float32)
            scales.append(jnp.exp2(0.25 * level) * (1.0 / 32767.0))
        for z in range(8):
            rows = pl.ds(z * length, length)
            total = jnp.zeros((length // 8, 8, 128), jnp.float32)
            for k in range(16):
                value = coded_ref[k, rows, :].astype(jnp.int32).astype(jnp.float32)
                total = total + value.reshape(length // 8, 8, 128) * scales[k]
            out_ref[z] = total.reshape(length, 128)

    return pl.pallas_call(
        kernel,
        compiler_params=LIMIT,
        in_specs=[VMEM],
        out_specs=VMEM,
        out_shape=jax.ShapeDtypeStruct((8, length, 128), jnp.float32),
    )(in_vmem(coded))


def part_kernel(where_ref, *refs):
    *cut_refs, out_ref, part_ref = refs
    for ref, (first, length) in zip(cut_refs, CUTS):
        total = ref[0]
        for k in range(1, 8):
            total = total + ref[k]
        part_ref[pl.ds(first, length), :] = total
    part = part_ref[...]
    row = lax.broadcasted_iota(jnp.int32, part.shape, 0)
    counted = (row >= SHARED) | (where_ref[0] % 2 == 0)
    total = jnp.sum(jnp.where(counted, part * part, 0.0))
    for k in range(8):
        out_ref[k, pl.ds(0, PART), :] = part
        out_ref[k, pl.ds(PART, 8), :] = jnp.full((8, 128), total, jnp.float32)


def part_sums(where, cuts):
    return pl.pallas_call(
        part_kernel,
        compiler_params=LIMIT,
        in_specs=[SMEM] + [VMEM] * len(cuts),
        out_specs=VMEM,
        out_shape=jax.ShapeDtypeStruct((8, PART + 8, 128), jnp.float32),
        scratch_shapes=[pltpu.VMEM((PART, 128), jnp.float32)],
    )(where, *map(in_vmem, cuts))


def column_kernel(where_ref, column_ref, out_ref):
    total = column_ref[0, pl.ds(PART, 8), :]
    for k in range(1, 8):
        total = total + column_ref[k, pl.ds(PART, 8), :]
    out_ref[pl.ds(0, PART), :] = column_ref[where_ref[2], pl.ds(0, PART), :]
    out_ref[pl.ds(PART, 8), :] = total


def column_total(where, column):
    return pl.pallas_call(
        column_kernel,
        compiler_params=LIMIT,
        in_specs=[SMEM, VMEM],
        out_specs=VMEM,
        out_shape=jax.ShapeDtypeStruct((PART + 8, 128), jnp.float32),
    )(where, in_vmem(column))


def chip_kernel(where_ref, mine_ref, theirs_ref, pair_ref, out_ref):
    first = where_ref[1] == 0
    mine, theirs = mine_ref[pl.ds(0, PART), :], theirs_ref[pl.ds(0, PART), :]
    pair_ref[0] = jnp.where(first, mine, theirs)
    pair_ref[1] = jnp.where(first, theirs, mine)
    total = mine_ref[pl.ds(PART, 8), :] + theirs_ref[pl.ds(PART, 8), :]
    for k in range(16):
        out_ref[k] = total


def chip_total(where, mine, theirs):
    return pl.pallas_call(
        chip_kernel,
        compiler_params=LIMIT,
        in_specs=[SMEM, VMEM, VMEM],
        out_specs=(VMEM, VMEM),
        out_shape=(
            jax.ShapeDtypeStruct((2, PART, 128), jnp.float32),
            jax.ShapeDtypeStruct((16, 8, 128), jnp.float32),
        ),
    )(where, in_vmem(mine), in_vmem(theirs))


def state_kernel(where_ref, *refs):
    *state_refs, out_ref = refs
    y, c = where_ref[0], where_ref[1]
    cols = pl.ds(pl.multiple_of((2 * c + y // 2) * 128, 128), 128)
    for k, ref in enumerate(state_refs):
        low, high = ref[pl.ds(0, PART), cols], ref[pl.ds(STARTS[1], PART), cols]
        part = jnp.where(y % 2 == 0, low, high)
        out_ref[k] = part


def state_parts(where, states):
    return pl.pallas_call(
        state_kernel,
        compiler_params=LIMIT,
        in_specs=[SMEM] + [VMEM] * 3,
        out_specs=VMEM,
        out_shape=jax.ShapeDtypeStruct((3, PART, 128), jnp.float32),
    )(where, *states)


def clip_of(totals_ref):
    total = totals_ref[0]
    for k in range(1, 16):
        total = total + totals_ref[k]
    norm = jnp.sqrt(total)
    return jnp.minimum(jnp.float32(1.0), 1.0 / (norm + 1e-06))[:1, :1]


def stepped(fixes_ref, clip, w, a, b, summed):
    gradient = clip * summed
    new_one = 0.9 * a + 0.1 * gradient
    new_two = 0.999 * b + 0.001 * gradient * gradient
    update = new_one / fixes_ref[0] / (jnp.sqrt(new_two / fixes_ref[1]) + 1e-08)
    return w - 0.01 * (update + 0.01 * w), new_one, new_two


def weights_kernel(where_ref, fixes_ref, totals_ref, column_ref, *refs):
    *state_refs, send_ref = refs
    clip = clip_of(totals_ref)
    for k, ref in enumerate(state_refs):
        z = (where_ref[2] + (8 - k)) % 8
        summed = column_ref[z, pl.ds(0, PART), :]
        part = stepped(fixes_ref, clip, ref[0], ref[1], ref[2], summed)[0].astype(jnp.bfloat16)
        rows = pl.ds(pl.multiple_of(z * PART, 8), PART)
        for j in range(16):
            send_ref[j, rows, :] = part


def new_weights(where, fixes, totals, column, states):
    return pl.pallas_call(
        weights_kernel,
        compiler_params=LIMIT,
        in_specs=[SMEM, SMEM] + [VMEM] * (2 + len(states)),
        out_specs=VMEM,
        out_shape=jax.ShapeDtypeStruct((16, 8 * PART, 128), jnp.bfloat16),
    )(where, fixes, in_vmem(totals), in_vmem(column), *map(in_vmem, states))


def own_kernel(where_ref, fixes_ref, totals_ref, *refs):
    pair_refs, (w_ref, a_ref, b_ref, w_out, a_out, b_out, summed) = refs[:4], refs[4:]
    for half in range(2):
        for y in (half, 2 + half):
            place = (where_ref[0] + (4 - y)) % 4
            for c in range(2):
                value = pair_refs[0][c]
                for k in range(1, 4):
                    value = jnp.where(place == k, pair_refs[k][c], value)
                summed[pl.ds(STARTS[half], PART), pl.ds((2 * c + y // 2) * 128, 128)] = value
    clip = clip_of(totals_ref)
    new = stepped(fixes_ref, clip, w_ref[...], a_ref[...], b_ref[...], summed[...])
    w_out[...], a_out[...], b_out[...] = new


def own_step(where, fixes, totals, pairs, states):
    rows = jax.ShapeDtypeStruct((108, 512), jnp.float32)
    return pl.pallas_call(
        own_kernel,
        compiler_params=LIMIT,
        in_specs=[SMEM, SMEM] + [VMEM] * 8,
        out_specs=(VMEM,) * 3,
        out_shape=(rows, rows, rows),
        scratch_shapes=[pltpu.VMEM((108, 512), jnp.float32)],
    )(where, fixes, in_vmem(totals), *map(in_vmem, pairs), *states)


def assemble_kernel(c_ref, mine_ref, theirs_ref, out_ref):
    x = pl.program_id(0)
    first = c_ref[0] == 0
    for half in range(2):
        for y in (half, 2 + half):
            for z in range(8):
                part = pl.ds(z * PART, PART)
                mine, theirs = mine_ref[x * 4 + y, part, :], theirs_ref[x * 4 + y, part, :]
                rows = pl.ds(108 * z + STARTS[half], PART)
                for c in range(2):
                    cols = pl.ds((2 * c + y // 2) * 128, 128)
                    out_ref[rows, cols] = jnp.where(first == (c == 0), mine, theirs)


def assemble(c, mine, theirs):
    return pl.pallas_call(
        assemble_kernel,
        compiler_params=LIMIT,
        grid_spec=pltpu.PrefetchScalarGridSpec(
            num_scalar_prefetch=1,
            grid=(4,),
            in_specs=[VMEM, VMEM],
            out_specs=pl.BlockSpec((864, 512), lambda i, c: (i, 0)),
        ),
        out_shape=jax.ShapeDtypeStruct((3456, 512), jnp.bfloat16),
    )(c, in_vmem(mine), in_vmem(theirs))


def shards(grads, master, moment_one, moment_two, step_count):
    y, c, z = (lax.axis_index(axis) for axis in ("y", "c", "z"))
    where = jnp.stack([y, c, z]).astype(jnp.int32)
    side = where[1:2]
    states = (master, moment_one, moment_two)
    steps = step_count[0].astype(jnp.float32)
    first_fix = 1.0 - jnp.power(jnp.float32(0.9), steps)
    second_fix = 1.0 - jnp.power(jnp.float32(0.999), steps)
    fixes = jnp.stack([first_fix, second_fix])
    local = grads[0, 0]
    theirs = swapped(lax.dynamic_slice(local, (0, 256 * (1 - c)), (3456, 256)), "c")
    state_columns = rotated(state_parts(where, states), "z")
    cuts = []
    for cut in CUTS:
        coded = exchanged(code_sums(side, local, theirs, cut), PLANE)
        coded, state_columns, fixes = lax.optimization_barrier((coded, state_columns, fixes))
        cuts.append(exchanged(sum_coded(coded, cut), "z"))
    column = exchanged(part_sums(where, cuts), "z")
    part = column_total(where, column)
    pair, total = chip_total(where, part, swapped(part, "c"))
    totals = exchanged(total, PLANE)
    mine = exchanged(new_weights(where, fixes, totals, column, state_columns), PLANE)
    own = own_step(where, fixes, totals, rotated(pair, "y"), states)
    mine, own = lax.optimization_barrier((mine, own))
    weights = assemble(side, mine, swapped(mine, "c"))
    return (*own, weights)


def solution(mesh):
    finer = Mesh(mesh.devices.reshape(4, 2, 4, 8), ("y", "c", "x", "z"))
    in_specs = (P(GRP, SHARD, None, None), P(SHARD, None), P(SHARD, None), P(SHARD, None), P())
    out_specs = (P(SHARD, None), P(SHARD, None), P(SHARD, None), P())
    return jax.shard_map(
        shards, mesh=finer, in_specs=in_specs, out_specs=out_specs, check_vma=False
    )
```

```python
import jax
import jax.numpy as jnp
from jax import lax
from jax.experimental import pallas as pl
from jax.experimental.pallas import tpu as pltpu
from jax.sharding import Mesh
from jax.sharding import PartitionSpec as P

GRP = ("y", "c")
SHARD = ("x", "z")
PLANE = ("x", "y")

PART = 56
STARTS = (0, 52)
SHARED = 4
COLUMN = 8 * PART
LIMIT = pltpu.CompilerParams(vmem_limit_bytes=24 * 2**20)
VMEM = pl.BlockSpec(memory_space=pltpu.VMEM)
ANY = pl.BlockSpec(memory_space=pl.ANY)
SMEM = pl.BlockSpec(memory_space=pltpu.SMEM)


def in_vmem(value):
    return pltpu.with_memory_space_constraint(value, pltpu.VMEM)


def exchanged(value, axes):
    return lax.all_to_all(value, axes, split_axis=0, concat_axis=0, tiled=True)


def swapped(value, axis):
    return lax.ppermute(value, axis, [(0, 1), (1, 0)])


def rotated(value, axis):
    n = lax.axis_size(axis)
    return [value] + [lax.ppermute(value, axis, [(i, (i + k) % n) for i in range(n)]) for k in range(1, n)]


def code_sums(c, local, theirs, piece, coded):
    def kernel(c_ref, mine_ref, theirs_ref, *refs):
        out_ref, sums = refs[-2:]
        for x, y in ((x, y) for x in range(2) for y in range(4)):
            lane = (y // 2) * 128
            mine_cols = pl.ds(pl.multiple_of(256 * c_ref[0] + lane, 128), 128)
            peak = jnp.zeros((8, 128), jnp.float32)
            for z in range(8):
                start = 864 * x + 108 * z + STARTS[y % 2]
                for t in range(0, PART, 8):
                    mine = mine_ref[pl.ds(1728 * piece + start + t, 8), mine_cols]
                    value = mine + theirs_ref[pl.ds(start + t, 8), pl.ds(lane, 128)]
                    peak = jnp.maximum(peak, jnp.abs(value))
                    sums[pl.ds(z * PART + t, 8), :] = value
            peak = jnp.max(peak, axis=0, keepdims=True)
            level = jnp.maximum(jnp.ceil(4.0 * jnp.log2(peak) + 0.02), -400.0)
            inverse = 32767.0 * jnp.exp2(-0.25 * level)
            for t in range(0, COLUMN, PART):
                scaled = jnp.round(sums[pl.ds(t, PART), :] * inverse)
                out_ref[x, y, pl.ds(t, PART), :] = scaled.astype(jnp.int32).astype(jnp.int16)
            level = jnp.broadcast_to(level, (8, 128))
            out_ref[x, y, pl.ds(COLUMN, 8), :] = level.astype(jnp.int32).astype(jnp.int16)

    return pl.pallas_call(
        kernel,
        compiler_params=LIMIT,
        grid_spec=pltpu.PrefetchScalarGridSpec(
            num_scalar_prefetch=1,
            grid=(1,),
            in_specs=[VMEM, VMEM] + [ANY] * len(coded),
            out_specs=pl.BlockSpec((2, 4, COLUMN + 8, 128), lambda i, c: (piece, 0, 0, 0)),
            scratch_shapes=[pltpu.VMEM((COLUMN, 128), jnp.float32)],
        ),
        out_shape=jax.ShapeDtypeStruct((4, 4, COLUMN + 8, 128), jnp.int16),
        input_output_aliases={3: 0} if coded else {},
    )(c, in_vmem(local), in_vmem(theirs), *coded)


def sum_kernel(coded_ref, out_ref):
    scales = []
    for k in range(16):
        level = coded_ref[k, pl.ds(COLUMN, 8), :].astype(jnp.int32).astype(jnp.float32)
        scales.append(jnp.exp2(0.25 * level) * (1.0 / 32767.0))
    for z in range(8):
        rows = pl.ds(z * PART, PART)
        total = jnp.zeros((PART // 8, 8, 128), jnp.float32)
        for k in range(16):
            value = coded_ref[k, rows, :].astype(jnp.int32).astype(jnp.float32)
            total = total + value.reshape(PART // 8, 8, 128) * scales[k]
        out_ref[z] = total.reshape(PART, 128)


def sum_coded(coded):
    return pl.pallas_call(
        sum_kernel,
        compiler_params=LIMIT,
        in_specs=[VMEM],
        out_specs=VMEM,
        out_shape=jax.ShapeDtypeStruct((8, PART, 128), jnp.float32),
    )(in_vmem(coded))


def part_kernel(where_ref, sums_ref, part_ref, out_ref):
    part = sums_ref[0]
    for k in range(1, 8):
        part = part + sums_ref[k]
    part_ref[...] = part
    row = lax.broadcasted_iota(jnp.int32, part.shape, 0)
    counted = (row >= SHARED) | (where_ref[0] % 2 == 0)
    total = jnp.sum(jnp.where(counted, part * part, 0.0))
    for k in range(8):
        out_ref[k, pl.ds(0, PART), :] = part
        out_ref[k, pl.ds(PART, 8), :] = jnp.full((8, 128), total, jnp.float32)


def part_sum(where, sums):
    return pl.pallas_call(
        part_kernel,
        compiler_params=LIMIT,
        in_specs=[SMEM, VMEM],
        out_specs=(VMEM, VMEM),
        out_shape=(
            jax.ShapeDtypeStruct((PART, 128), jnp.float32),
            jax.ShapeDtypeStruct((8, PART + 8, 128), jnp.float32),
        ),
    )(where, in_vmem(sums))


def column_kernel(column_ref, *refs):
    *part_refs, out_ref = refs
    total = column_ref[0, pl.ds(PART, 8), :]
    for k in range(1, 8):
        total = total + column_ref[k, pl.ds(PART, 8), :]
    for k, ref in enumerate(part_refs):
        out_ref[pl.ds(k * PART, PART), :] = ref[...]
    out_ref[pl.ds(4 * PART, 8), :] = total


def column_total(column, parts):
    return pl.pallas_call(
        column_kernel,
        compiler_params=LIMIT,
        in_specs=[VMEM] * 5,
        out_specs=VMEM,
        out_shape=jax.ShapeDtypeStruct((4 * PART + 8, 128), jnp.float32),
    )(*map(in_vmem, (column, *parts)))


def chip_kernel(mine_ref, theirs_ref, out_ref):
    total = mine_ref[pl.ds(4 * PART, 8), :] + theirs_ref[pl.ds(4 * PART, 8), :]
    for k in range(16):
        out_ref[k] = total


def chip_total(mine, theirs):
    return pl.pallas_call(
        chip_kernel,
        compiler_params=LIMIT,
        in_specs=[VMEM, VMEM],
        out_specs=VMEM,
        out_shape=jax.ShapeDtypeStruct((16, 8, 128), jnp.float32),
    )(in_vmem(mine), in_vmem(theirs))


def state_kernel(where_ref, *refs):
    *state_refs, out_ref = refs
    y, c = where_ref[0], where_ref[1]
    cols = pl.ds(pl.multiple_of((2 * c + y // 2) * 128, 128), 128)
    for k, ref in enumerate(state_refs):
        low, high = ref[pl.ds(0, PART), cols], ref[pl.ds(STARTS[1], PART), cols]
        part = jnp.where(y % 2 == 0, low, high)
        out_ref[k] = part


def state_parts(where, states):
    return pl.pallas_call(
        state_kernel,
        compiler_params=LIMIT,
        in_specs=[SMEM] + [VMEM] * 3,
        out_specs=VMEM,
        out_shape=jax.ShapeDtypeStruct((3, PART, 128), jnp.float32),
    )(where, *states)


def clip_of(totals_ref):
    total = totals_ref[0]
    for k in range(1, 16):
        total = total + totals_ref[k]
    norm = jnp.sqrt(total)
    return jnp.minimum(jnp.float32(1.0), 1.0 / (norm + 1e-06))[:1, :1]


def stepped(fixes_ref, clip, w, a, b, summed):
    gradient = clip * summed
    new_one = 0.9 * a + 0.1 * gradient
    new_two = 0.999 * b + 0.001 * gradient * gradient
    update = new_one / fixes_ref[0] / (jnp.sqrt(new_two / fixes_ref[1]) + 1e-08)
    return w - 0.01 * (update + 0.01 * w), new_one, new_two


def weights_kernel(where_ref, fixes_ref, totals_ref, column_ref, *refs):
    *state_refs, send_ref = refs
    clip = clip_of(totals_ref)
    for k, ref in enumerate(state_refs):
        z = (where_ref[2] + (8 - k)) % 8
        summed = column_ref[z, pl.ds(0, PART), :]
        part = stepped(fixes_ref, clip, ref[0], ref[1], ref[2], summed)[0].astype(jnp.bfloat16)
        rows = pl.ds(pl.multiple_of(z * PART, 8), PART)
        for j in range(16):
            send_ref[j, rows, :] = part


def new_weights(where, fixes, totals, column, states):
    return pl.pallas_call(
        weights_kernel,
        compiler_params=LIMIT,
        in_specs=[SMEM, SMEM] + [VMEM] * (2 + len(states)),
        out_specs=VMEM,
        out_shape=jax.ShapeDtypeStruct((16, 8 * PART, 128), jnp.bfloat16),
    )(where, fixes, in_vmem(totals), in_vmem(column), *map(in_vmem, states))


def own_kernel(where_ref, fixes_ref, totals_ref, mine_ref, theirs_ref, *refs):
    w_ref, a_ref, b_ref, w_out, a_out, b_out, summed = refs
    for half in range(2):
        for y in (half, 2 + half):
            place = (where_ref[0] + (4 - y)) % 4
            rows = pl.ds(pl.multiple_of(place * PART, 8), PART)
            mine, theirs = mine_ref[rows, :], theirs_ref[rows, :]
            for c in range(2):
                value = jnp.where(where_ref[1] == c, mine, theirs)
                summed[pl.ds(STARTS[half], PART), pl.ds((2 * c + y // 2) * 128, 128)] = value
    clip = clip_of(totals_ref)
    new = stepped(fixes_ref, clip, w_ref[...], a_ref[...], b_ref[...], summed[...])
    w_out[...], a_out[...], b_out[...] = new


def own_step(where, fixes, totals, mine, theirs, states):
    rows = jax.ShapeDtypeStruct((108, 512), jnp.float32)
    return pl.pallas_call(
        own_kernel,
        compiler_params=LIMIT,
        in_specs=[SMEM, SMEM] + [VMEM] * 6,
        out_specs=(VMEM,) * 3,
        out_shape=(rows, rows, rows),
        scratch_shapes=[pltpu.VMEM((108, 512), jnp.float32)],
    )(where, fixes, *map(in_vmem, (totals, mine, theirs)), *states)


def assemble(c, mine, theirs, piece, weights):
    def kernel(c_ref, mine_ref, theirs_ref, *refs):
        out_ref = refs[-1]
        first = c_ref[0] == 0
        for half in range(2):
            for x, y in ((x, y) for x in range(2) for y in (half, 2 + half)):
                for z in range(8):
                    part = pl.ds(z * PART, PART)
                    own, other = mine_ref[8 * piece + 4 * x + y, part, :], theirs_ref[4 * x + y, part, :]
                    rows = pl.ds(864 * x + 108 * z + STARTS[half], PART)
                    for c in range(2):
                        cols = pl.ds((2 * c + y // 2) * 128, 128)
                        out_ref[rows, cols] = jnp.where(first == (c == 0), own, other)

    return pl.pallas_call(
        kernel,
        compiler_params=LIMIT,
        grid_spec=pltpu.PrefetchScalarGridSpec(
            num_scalar_prefetch=1,
            grid=(1,),
            in_specs=[VMEM, VMEM] + [ANY] * len(weights),
            out_specs=pl.BlockSpec((1728, 512), lambda i, c: (piece, 0)),
        ),
        out_shape=jax.ShapeDtypeStruct((3456, 512), jnp.bfloat16),
        input_output_aliases={3: 0} if weights else {},
    )(c, in_vmem(mine), in_vmem(theirs), *weights)


def shards(grads, master, moment_one, moment_two, step_count):
    y, c, z = (lax.axis_index(axis) for axis in ("y", "c", "z"))
    where = jnp.stack([y, c, z]).astype(jnp.int32)
    side = where[1:2]
    states = (master, moment_one, moment_two)
    steps = step_count[0].astype(jnp.float32)
    first_fix = 1.0 - jnp.power(jnp.float32(0.9), steps)
    second_fix = 1.0 - jnp.power(jnp.float32(0.999), steps)
    fixes = jnp.stack([first_fix, second_fix])
    local = grads[0, 0]
    theirs = [swapped(lax.dynamic_slice(local, (1728 * k, 256 * (1 - c)), (1728, 256)), "c") for k in range(2)]
    coded = ()
    for k in range(2):
        coded = (code_sums(side, local, theirs[k], k, coded),)
    coded = exchanged(coded[0].reshape(16, COLUMN + 8, 128), PLANE)
    state_columns = rotated(state_parts(where, states), "z")
    coded, state_columns, fixes = lax.optimization_barrier((coded, state_columns, fixes))
    part, sent = part_sum(where, exchanged(sum_coded(coded), "z"))
    column = exchanged(sent, "z")
    own = column_total(column, rotated(part, "y"))
    other = swapped(own, "c")
    totals = exchanged(chip_total(own, other), PLANE)
    mine = exchanged(new_weights(where, fixes, totals, column, state_columns), PLANE)
    new = own_step(where, fixes, totals, own, other, states)
    theirs = [swapped(mine[8 * k : 8 * k + 8], "c") for k in range(2)]
    weights = ()
    for k in range(2):
        weights = (assemble(side, mine, theirs[k], k, weights),)
    return (*new, *weights)


def solution(mesh):
    finer = Mesh(mesh.devices.reshape(4, 2, 4, 8), ("y", "c", "x", "z"))
    in_specs = (P(GRP, SHARD, None, None), P(SHARD, None), P(SHARD, None), P(SHARD, None), P())
    out_specs = (P(SHARD, None), P(SHARD, None), P(SHARD, None), P())
    return jax.shard_map(
        shards, mesh=finer, in_specs=in_specs, out_specs=out_specs, check_vma=False
    )
```

```python
import jax
import jax.numpy as jnp
from jax import lax
from jax.experimental import pallas as pl
from jax.experimental.pallas import tpu as pltpu
from jax.sharding import Mesh
from jax.sharding import PartitionSpec as P

GRP = ("y", "c")
SHARD = ("x", "z")
PLANE = ("x", "y")

PART = 56
STARTS = (0, 52)
SHARED = 4
COLUMN = 8 * PART
LIMIT = pltpu.CompilerParams(vmem_limit_bytes=24 * 2**20)
VMEM = pl.BlockSpec(memory_space=pltpu.VMEM)
ANY = pl.BlockSpec(memory_space=pl.ANY)
SMEM = pl.BlockSpec(memory_space=pltpu.SMEM)


def in_vmem(value):
    return pltpu.with_memory_space_constraint(value, pltpu.VMEM)


def in_hbm(value):
    return pltpu.with_memory_space_constraint(value, pltpu.HBM)


def exchanged(value, axes):
    return lax.all_to_all(value, axes, split_axis=0, concat_axis=0, tiled=True)


def swapped(value, axis):
    return lax.ppermute(value, axis, [(0, 1), (1, 0)])


def rotated(value, axis):
    n = lax.axis_size(axis)
    return [value] + [lax.ppermute(value, axis, [(i, (i + k) % n) for i in range(n)]) for k in range(1, n)]


def scale_of(level):
    return jnp.exp2(0.25 * level.astype(jnp.int32).astype(jnp.float32)) * (1.0 / 32767.0)


def coded_block(value):
    peak = jnp.max(jnp.abs(value), axis=0, keepdims=True)
    level = jnp.maximum(jnp.ceil(4.0 * jnp.log2(peak) + 0.02), -400.0)
    scaled = jnp.round(value * (32767.0 * jnp.exp2(-0.25 * level)))
    return scaled.astype(jnp.int32).astype(jnp.int16), level


def decoded(block, scale):
    return block.astype(jnp.int32).astype(jnp.float32) * scale


def code(out_ref, value_of):
    row = lax.broadcasted_iota(jnp.int32, (8, 128), 0)
    levels = jnp.zeros((8, 128), jnp.float32)
    for z in range(8):
        block, level = coded_block(value_of(z))
        levels = jnp.where(row == z, level, levels)
        out_ref[pl.ds(z * PART, PART), :] = block
    out_ref[pl.ds(COLUMN, 8), :] = levels.astype(jnp.int32).astype(jnp.int16)


def half_kernel(c_ref, local_ref, out_ref):
    for y in range(4):
        cols = pl.ds((y // 2) * 128, 128)
        code(out_ref.at[0, y], lambda z: local_ref[pl.ds(108 * z + STARTS[y % 2], PART), cols])


def code_half(c, local, piece):
    return pl.pallas_call(
        half_kernel,
        compiler_params=LIMIT,
        grid_spec=pltpu.PrefetchScalarGridSpec(
            num_scalar_prefetch=1,
            grid=(2,),
            in_specs=[pl.BlockSpec((864, 256), lambda i, c: (2 * piece + i, 1 - c[0]))],
            out_specs=pl.BlockSpec((1, 4, COLUMN + 8, 128), lambda i, c: (i, 0, 0, 0)),
        ),
        out_shape=jax.ShapeDtypeStruct((2, 4, COLUMN + 8, 128), jnp.int16),
    )(c, in_hbm(local))


def code_sums(c, local, theirs, piece, coded):
    def kernel(c_ref, mine_ref, theirs_ref, *refs):
        out_ref = refs[-1]
        for x, y in ((x, y) for x in range(2) for y in range(4)):
            cols = pl.ds(pl.multiple_of(256 * c_ref[0] + (y // 2) * 128, 128), 128)
            scales = scale_of(theirs_ref[x, y, pl.ds(COLUMN, 8), :])

            def value_of(z):
                mine = mine_ref[pl.ds(1728 * piece + 864 * x + 108 * z + STARTS[y % 2], PART), cols]
                return mine + decoded(theirs_ref[x, y, pl.ds(z * PART, PART), :], scales[z : z + 1])

            code(out_ref.at[x, y], value_of)

    return pl.pallas_call(
        kernel,
        compiler_params=LIMIT,
        grid_spec=pltpu.PrefetchScalarGridSpec(
            num_scalar_prefetch=1,
            grid=(1,),
            in_specs=[VMEM, VMEM] + [ANY] * len(coded),
            out_specs=pl.BlockSpec((2, 4, COLUMN + 8, 128), lambda i, c: (piece, 0, 0, 0)),
        ),
        out_shape=jax.ShapeDtypeStruct((4, 4, COLUMN + 8, 128), jnp.int16),
        input_output_aliases={3: 0} if coded else {},
    )(c, in_vmem(local), in_vmem(theirs), *coded)


def sum_kernel(coded_ref, out_ref):
    scales = [scale_of(coded_ref[k, pl.ds(COLUMN, 8), :]) for k in range(16)]
    for z in range(8):
        rows = pl.ds(z * PART, PART)
        total = jnp.zeros((PART, 128), jnp.float32)
        for k in range(16):
            total = total + decoded(coded_ref[k, rows, :], scales[k][z : z + 1])
        block, level = coded_block(total)
        out_ref[z, pl.ds(0, PART), :] = block
        level = jnp.broadcast_to(level, (8, 128))
        out_ref[z, pl.ds(PART, 8), :] = level.astype(jnp.int32).astype(jnp.int16)


def sum_coded(coded):
    return pl.pallas_call(
        sum_kernel,
        compiler_params=LIMIT,
        in_specs=[VMEM],
        out_specs=VMEM,
        out_shape=jax.ShapeDtypeStruct((8, PART + 8, 128), jnp.int16),
    )(in_vmem(coded))


def part_kernel(where_ref, sums_ref, part_ref, out_ref):
    part = jnp.zeros((PART, 128), jnp.float32)
    for k in range(8):
        scale = scale_of(sums_ref[k, pl.ds(PART, 8), :])[:1]
        part = part + decoded(sums_ref[k, pl.ds(0, PART), :], scale)
    part_ref[...] = part
    row = lax.broadcasted_iota(jnp.int32, part.shape, 0)
    counted = (row >= SHARED) | (where_ref[0] % 2 == 0)
    total = jnp.sum(jnp.where(counted, part * part, 0.0))
    for k in range(8):
        out_ref[k, pl.ds(0, PART), :] = part
        out_ref[k, pl.ds(PART, 8), :] = jnp.full((8, 128), total, jnp.float32)


def part_sum(where, sums):
    return pl.pallas_call(
        part_kernel,
        compiler_params=LIMIT,
        in_specs=[SMEM, VMEM],
        out_specs=(VMEM, VMEM),
        out_shape=(
            jax.ShapeDtypeStruct((PART, 128), jnp.float32),
            jax.ShapeDtypeStruct((8, PART + 8, 128), jnp.float32),
        ),
    )(where, in_vmem(sums))


def column_kernel(column_ref, *refs):
    *part_refs, out_ref = refs
    total = column_ref[0, pl.ds(PART, 8), :]
    for k in range(1, 8):
        total = total + column_ref[k, pl.ds(PART, 8), :]
    for k, ref in enumerate(part_refs):
        out_ref[pl.ds(k * PART, PART), :] = ref[...]
    out_ref[pl.ds(4 * PART, 8), :] = total


def column_total(column, parts):
    return pl.pallas_call(
        column_kernel,
        compiler_params=LIMIT,
        in_specs=[VMEM] * 5,
        out_specs=VMEM,
        out_shape=jax.ShapeDtypeStruct((4 * PART + 8, 128), jnp.float32),
    )(*map(in_vmem, (column, *parts)))


def chip_kernel(mine_ref, theirs_ref, out_ref):
    total = mine_ref[pl.ds(4 * PART, 8), :] + theirs_ref[pl.ds(4 * PART, 8), :]
    for k in range(16):
        out_ref[k] = total


def chip_total(mine, theirs):
    return pl.pallas_call(
        chip_kernel,
        compiler_params=LIMIT,
        in_specs=[VMEM, VMEM],
        out_specs=VMEM,
        out_shape=jax.ShapeDtypeStruct((16, 8, 128), jnp.float32),
    )(in_vmem(mine), in_vmem(theirs))


def state_kernel(where_ref, *refs):
    *state_refs, out_ref = refs
    y, c = where_ref[0], where_ref[1]
    cols = pl.ds(pl.multiple_of((2 * c + y // 2) * 128, 128), 128)
    for k, ref in enumerate(state_refs):
        low, high = ref[pl.ds(0, PART), cols], ref[pl.ds(STARTS[1], PART), cols]
        part = jnp.where(y % 2 == 0, low, high)
        out_ref[k] = part


def state_parts(where, states):
    return pl.pallas_call(
        state_kernel,
        compiler_params=LIMIT,
        in_specs=[SMEM] + [VMEM] * 3,
        out_specs=VMEM,
        out_shape=jax.ShapeDtypeStruct((3, PART, 128), jnp.float32),
    )(where, *states)


def clip_of(totals_ref):
    total = totals_ref[0]
    for k in range(1, 16):
        total = total + totals_ref[k]
    norm = jnp.sqrt(total)
    return jnp.minimum(jnp.float32(1.0), 1.0 / (norm + 1e-06))[:1, :1]


def stepped(fixes_ref, clip, w, a, b, summed):
    gradient = clip * summed
    new_one = 0.9 * a + 0.1 * gradient
    new_two = 0.999 * b + 0.001 * gradient * gradient
    update = new_one / fixes_ref[0] / (jnp.sqrt(new_two / fixes_ref[1]) + 1e-08)
    return w - 0.01 * (update + 0.01 * w), new_one, new_two


def weights_kernel(where_ref, fixes_ref, totals_ref, column_ref, *refs):
    *state_refs, send_ref = refs
    clip = clip_of(totals_ref)
    for k, ref in enumerate(state_refs):
        z = (where_ref[2] + (8 - k)) % 8
        summed = column_ref[z, pl.ds(0, PART), :]
        part = stepped(fixes_ref, clip, ref[0], ref[1], ref[2], summed)[0].astype(jnp.bfloat16)
        rows = pl.ds(pl.multiple_of(z * PART, 8), PART)
        for j in range(16):
            send_ref[j, rows, :] = part


def new_weights(where, fixes, totals, column, states):
    return pl.pallas_call(
        weights_kernel,
        compiler_params=LIMIT,
        in_specs=[SMEM, SMEM] + [VMEM] * (2 + len(states)),
        out_specs=VMEM,
        out_shape=jax.ShapeDtypeStruct((16, 8 * PART, 128), jnp.bfloat16),
    )(where, fixes, in_vmem(totals), in_vmem(column), *map(in_vmem, states))


def own_kernel(where_ref, fixes_ref, totals_ref, mine_ref, theirs_ref, *refs):
    w_ref, a_ref, b_ref, w_out, a_out, b_out, summed = refs
    for half in range(2):
        for y in (half, 2 + half):
            place = (where_ref[0] + (4 - y)) % 4
            rows = pl.ds(pl.multiple_of(place * PART, 8), PART)
            mine, theirs = mine_ref[rows, :], theirs_ref[rows, :]
            for c in range(2):
                value = jnp.where(where_ref[1] == c, mine, theirs)
                summed[pl.ds(STARTS[half], PART), pl.ds((2 * c + y // 2) * 128, 128)] = value
    clip = clip_of(totals_ref)
    new = stepped(fixes_ref, clip, w_ref[...], a_ref[...], b_ref[...], summed[...])
    w_out[...], a_out[...], b_out[...] = new


def own_step(where, fixes, totals, mine, theirs, states):
    rows = jax.ShapeDtypeStruct((108, 512), jnp.float32)
    return pl.pallas_call(
        own_kernel,
        compiler_params=LIMIT,
        in_specs=[SMEM, SMEM] + [VMEM] * 6,
        out_specs=(VMEM,) * 3,
        out_shape=(rows, rows, rows),
        scratch_shapes=[pltpu.VMEM((108, 512), jnp.float32)],
    )(where, fixes, *map(in_vmem, (totals, mine, theirs)), *states)


def assemble(c, mine, theirs, piece, weights):
    def kernel(c_ref, mine_ref, theirs_ref, *refs):
        out_ref = refs[-1]
        first = c_ref[0] == 0
        for half in range(2):
            for x, y in ((x, y) for x in range(2) for y in (half, 2 + half)):
                for z in range(8):
                    part = pl.ds(z * PART, PART)
                    own, other = mine_ref[8 * piece + 4 * x + y, part, :], theirs_ref[4 * x + y, part, :]
                    rows = pl.ds(864 * x + 108 * z + STARTS[half], PART)
                    for c in range(2):
                        cols = pl.ds((2 * c + y // 2) * 128, 128)
                        out_ref[rows, cols] = jnp.where(first == (c == 0), own, other)

    return pl.pallas_call(
        kernel,
        compiler_params=LIMIT,
        grid_spec=pltpu.PrefetchScalarGridSpec(
            num_scalar_prefetch=1,
            grid=(1,),
            in_specs=[VMEM, VMEM] + [ANY] * len(weights),
            out_specs=pl.BlockSpec((1728, 512), lambda i, c: (piece, 0)),
        ),
        out_shape=jax.ShapeDtypeStruct((3456, 512), jnp.bfloat16),
        input_output_aliases={3: 0} if weights else {},
    )(c, in_vmem(mine), in_vmem(theirs), *weights)


def shards(grads, master, moment_one, moment_two, step_count):
    y, c, z = (lax.axis_index(axis) for axis in ("y", "c", "z"))
    where = jnp.stack([y, c, z]).astype(jnp.int32)
    side = where[1:2]
    states = (master, moment_one, moment_two)
    steps = step_count[0].astype(jnp.float32)
    first_fix = 1.0 - jnp.power(jnp.float32(0.9), steps)
    second_fix = 1.0 - jnp.power(jnp.float32(0.999), steps)
    fixes = jnp.stack([first_fix, second_fix])
    local = grads[0, 0]
    theirs = [swapped(code_half(side, local, k), "c") for k in range(2)]
    coded = ()
    for k in range(2):
        coded = (code_sums(side, local, theirs[k], k, coded),)
    coded = exchanged(coded[0].reshape(16, COLUMN + 8, 128), PLANE)
    state_columns = rotated(state_parts(where, states), "z")
    coded, state_columns, fixes = lax.optimization_barrier((coded, state_columns, fixes))
    part, sent = part_sum(where, exchanged(sum_coded(coded), "z"))
    column = exchanged(sent, "z")
    own = column_total(column, rotated(part, "y"))
    other = swapped(own, "c")
    totals = exchanged(chip_total(own, other), PLANE)
    mine = exchanged(new_weights(where, fixes, totals, column, state_columns), PLANE)
    new = own_step(where, fixes, totals, own, other, states)
    theirs = [swapped(mine[8 * k : 8 * k + 8], "c") for k in range(2)]
    weights = ()
    for k in range(2):
        weights = (assemble(side, mine, theirs[k], k, weights),)
    return (*new, *weights)


def solution(mesh):
    finer = Mesh(mesh.devices.reshape(4, 2, 4, 8), ("y", "c", "x", "z"))
    in_specs = (P(GRP, SHARD, None, None), P(SHARD, None), P(SHARD, None), P(SHARD, None), P())
    out_specs = (P(SHARD, None), P(SHARD, None), P(SHARD, None), P())
    return jax.shard_map(
        shards, mesh=finer, in_specs=in_specs, out_specs=out_specs, check_vma=False
    )
```

```python
import jax
import jax.numpy as jnp
from jax import lax
from jax.experimental import pallas as pl
from jax.experimental.pallas import tpu as pltpu
from jax.sharding import Mesh
from jax.sharding import PartitionSpec as P

GRP = ("y", "c")
SHARD = ("x", "z")
PLANE = ("x", "y")

PART = 56
STARTS = (0, 52)
SHARED = 4
COLUMN = 8 * PART
LIMIT = pltpu.CompilerParams(vmem_limit_bytes=24 * 2**20)
VMEM = pl.BlockSpec(memory_space=pltpu.VMEM)
ANY = pl.BlockSpec(memory_space=pl.ANY)
SMEM = pl.BlockSpec(memory_space=pltpu.SMEM)


def in_vmem(value):
    return pltpu.with_memory_space_constraint(value, pltpu.VMEM)


def in_hbm(value):
    return pltpu.with_memory_space_constraint(value, pltpu.HBM)


def exchanged(value, axes):
    return lax.all_to_all(value, axes, split_axis=0, concat_axis=0, tiled=True)


def swapped(value, axis):
    return lax.ppermute(value, axis, [(0, 1), (1, 0)])


def rotated(value, axis):
    n = lax.axis_size(axis)
    return [value] + [lax.ppermute(value, axis, [(i, (i + k) % n) for i in range(n)]) for k in range(1, n)]


def scale_of(level):
    return jnp.exp2(0.0625 * level.astype(jnp.int32).astype(jnp.float32)) * (1.0 / 32767.0)


def coded_block(value):
    peak = jnp.max(jnp.abs(value), axis=0, keepdims=True)
    level = jnp.maximum(jnp.ceil(16.0 * jnp.log2(peak) + 0.02), -1600.0)
    scaled = jnp.round(value * (32767.0 * jnp.exp2(-0.0625 * level)))
    return scaled.astype(jnp.int32).astype(jnp.int16), level


def decoded(block, scale):
    return block.astype(jnp.int32).astype(jnp.float32) * scale


def code(out_ref, value_of):
    row = lax.broadcasted_iota(jnp.int32, (8, 128), 0)
    levels = jnp.zeros((8, 128), jnp.float32)
    for z in range(8):
        block, level = coded_block(value_of(z))
        levels = jnp.where(row == z, level, levels)
        out_ref[pl.ds(z * PART, PART), :] = block
    out_ref[pl.ds(COLUMN, 8), :] = levels.astype(jnp.int32).astype(jnp.int16)


def half_kernel(c_ref, local_ref, out_ref):
    for y in range(4):
        cols = pl.ds((y // 2) * 128, 128)
        code(out_ref.at[0, y], lambda z: local_ref[pl.ds(108 * z + STARTS[y % 2], PART), cols])


def code_half(c, local, piece):
    return pl.pallas_call(
        half_kernel,
        compiler_params=LIMIT,
        grid_spec=pltpu.PrefetchScalarGridSpec(
            num_scalar_prefetch=1,
            grid=(2,),
            in_specs=[pl.BlockSpec((864, 256), lambda i, c: (2 * piece + i, 1 - c[0]))],
            out_specs=pl.BlockSpec((1, 4, COLUMN + 8, 128), lambda i, c: (i, 0, 0, 0)),
        ),
        out_shape=jax.ShapeDtypeStruct((2, 4, COLUMN + 8, 128), jnp.int16),
    )(c, in_hbm(local))


def code_sums(c, local, theirs, piece, coded):
    def kernel(c_ref, mine_ref, theirs_ref, *refs):
        out_ref = refs[-1]
        for x, y in ((x, y) for x in range(2) for y in range(4)):
            cols = pl.ds(pl.multiple_of(256 * c_ref[0] + (y // 2) * 128, 128), 128)
            scales = scale_of(theirs_ref[x, y, pl.ds(COLUMN, 8), :])

            def value_of(z):
                mine = mine_ref[pl.ds(1728 * piece + 864 * x + 108 * z + STARTS[y % 2], PART), cols]
                return mine + decoded(theirs_ref[x, y, pl.ds(z * PART, PART), :], scales[z : z + 1])

            code(out_ref.at[x, y], value_of)

    return pl.pallas_call(
        kernel,
        compiler_params=LIMIT,
        grid_spec=pltpu.PrefetchScalarGridSpec(
            num_scalar_prefetch=1,
            grid=(1,),
            in_specs=[VMEM, VMEM] + [ANY] * len(coded),
            out_specs=pl.BlockSpec((2, 4, COLUMN + 8, 128), lambda i, c: (piece, 0, 0, 0)),
        ),
        out_shape=jax.ShapeDtypeStruct((4, 4, COLUMN + 8, 128), jnp.int16),
        input_output_aliases={3: 0} if coded else {},
    )(c, in_vmem(local), in_vmem(theirs), *coded)


def sum_kernel(coded_ref, out_ref):
    scales = [scale_of(coded_ref[k, pl.ds(COLUMN, 8), :]) for k in range(16)]
    for z in range(8):
        rows = pl.ds(z * PART, PART)
        total = jnp.zeros((PART, 128), jnp.float32)
        for k in range(16):
            total = total + decoded(coded_ref[k, rows, :], scales[k][z : z + 1])
        block, level = coded_block(total)
        out_ref[z, pl.ds(0, PART), :] = block
        level = jnp.broadcast_to(level, (8, 128))
        out_ref[z, pl.ds(PART, 8), :] = level.astype(jnp.int32).astype(jnp.int16)


def sum_coded(coded):
    return pl.pallas_call(
        sum_kernel,
        compiler_params=LIMIT,
        in_specs=[VMEM],
        out_specs=VMEM,
        out_shape=jax.ShapeDtypeStruct((8, PART + 8, 128), jnp.int16),
    )(in_vmem(coded))


def part_kernel(where_ref, sums_ref, part_ref, out_ref):
    part = jnp.zeros((PART, 128), jnp.float32)
    for k in range(8):
        scale = scale_of(sums_ref[k, pl.ds(PART, 8), :])[:1]
        part = part + decoded(sums_ref[k, pl.ds(0, PART), :], scale)
    part_ref[...] = part
    row = lax.broadcasted_iota(jnp.int32, part.shape, 0)
    counted = (row >= SHARED) | (where_ref[0] % 2 == 0)
    total = jnp.sum(jnp.where(counted, part * part, 0.0))
    for k in range(8):
        out_ref[k, pl.ds(0, PART), :] = part
        out_ref[k, pl.ds(PART, 8), :] = jnp.full((8, 128), total, jnp.float32)


def part_sum(where, sums):
    return pl.pallas_call(
        part_kernel,
        compiler_params=LIMIT,
        in_specs=[SMEM, VMEM],
        out_specs=(VMEM, VMEM),
        out_shape=(
            jax.ShapeDtypeStruct((PART, 128), jnp.float32),
            jax.ShapeDtypeStruct((8, PART + 8, 128), jnp.float32),
        ),
    )(where, in_vmem(sums))


def column_kernel(column_ref, *refs):
    *part_refs, out_ref = refs
    total = column_ref[0, pl.ds(PART, 8), :]
    for k in range(1, 8):
        total = total + column_ref[k, pl.ds(PART, 8), :]
    for k, ref in enumerate(part_refs):
        out_ref[pl.ds(k * PART, PART), :] = ref[...]
    out_ref[pl.ds(4 * PART, 8), :] = total


def column_total(column, parts):
    return pl.pallas_call(
        column_kernel,
        compiler_params=LIMIT,
        in_specs=[VMEM] * 5,
        out_specs=VMEM,
        out_shape=jax.ShapeDtypeStruct((4 * PART + 8, 128), jnp.float32),
    )(*map(in_vmem, (column, *parts)))


def chip_kernel(mine_ref, theirs_ref, out_ref):
    total = mine_ref[pl.ds(4 * PART, 8), :] + theirs_ref[pl.ds(4 * PART, 8), :]
    for k in range(16):
        out_ref[k] = total


def chip_total(mine, theirs):
    return pl.pallas_call(
        chip_kernel,
        compiler_params=LIMIT,
        in_specs=[VMEM, VMEM],
        out_specs=VMEM,
        out_shape=jax.ShapeDtypeStruct((16, 8, 128), jnp.float32),
    )(in_vmem(mine), in_vmem(theirs))


def state_kernel(where_ref, *refs):
    *state_refs, out_ref = refs
    y, c = where_ref[0], where_ref[1]
    cols = pl.ds(pl.multiple_of((2 * c + y // 2) * 128, 128), 128)
    for k, ref in enumerate(state_refs):
        low, high = ref[pl.ds(0, PART), cols], ref[pl.ds(STARTS[1], PART), cols]
        part = jnp.where(y % 2 == 0, low, high)
        out_ref[k] = part


def state_parts(where, states):
    return pl.pallas_call(
        state_kernel,
        compiler_params=LIMIT,
        in_specs=[SMEM] + [VMEM] * 3,
        out_specs=VMEM,
        out_shape=jax.ShapeDtypeStruct((3, PART, 128), jnp.float32),
    )(where, *states)


def clip_of(totals_ref):
    total = totals_ref[0]
    for k in range(1, 16):
        total = total + totals_ref[k]
    norm = jnp.sqrt(total)
    return jnp.minimum(jnp.float32(1.0), 1.0 / (norm + 1e-06))[:1, :1]


def stepped(fixes_ref, clip, w, a, b, summed):
    gradient = clip * summed
    new_one = 0.9 * a + 0.1 * gradient
    new_two = 0.999 * b + 0.001 * gradient * gradient
    update = new_one / fixes_ref[0] / (jnp.sqrt(new_two / fixes_ref[1]) + 1e-08)
    return w - 0.01 * (update + 0.01 * w), new_one, new_two


def weights_kernel(where_ref, fixes_ref, totals_ref, column_ref, *refs):
    *state_refs, send_ref = refs
    clip = clip_of(totals_ref)
    for k, ref in enumerate(state_refs):
        z = (where_ref[2] + (8 - k)) % 8
        summed = column_ref[z, pl.ds(0, PART), :]
        part = stepped(fixes_ref, clip, ref[0], ref[1], ref[2], summed)[0].astype(jnp.bfloat16)
        rows = pl.ds(pl.multiple_of(z * PART, 8), PART)
        for j in range(16):
            send_ref[j, rows, :] = part


def new_weights(where, fixes, totals, column, states):
    return pl.pallas_call(
        weights_kernel,
        compiler_params=LIMIT,
        in_specs=[SMEM, SMEM] + [VMEM] * (2 + len(states)),
        out_specs=VMEM,
        out_shape=jax.ShapeDtypeStruct((16, 8 * PART, 128), jnp.bfloat16),
    )(where, fixes, in_vmem(totals), in_vmem(column), *map(in_vmem, states))


def own_kernel(where_ref, fixes_ref, totals_ref, mine_ref, theirs_ref, *refs):
    w_ref, a_ref, b_ref, w_out, a_out, b_out, summed = refs
    for half in range(2):
        for y in (half, 2 + half):
            place = (where_ref[0] + (4 - y)) % 4
            rows = pl.ds(pl.multiple_of(place * PART, 8), PART)
            mine, theirs = mine_ref[rows, :], theirs_ref[rows, :]
            for c in range(2):
                value = jnp.where(where_ref[1] == c, mine, theirs)
                summed[pl.ds(STARTS[half], PART), pl.ds((2 * c + y // 2) * 128, 128)] = value
    clip = clip_of(totals_ref)
    new = stepped(fixes_ref, clip, w_ref[...], a_ref[...], b_ref[...], summed[...])
    w_out[...], a_out[...], b_out[...] = new


def own_step(where, fixes, totals, mine, theirs, states):
    rows = jax.ShapeDtypeStruct((108, 512), jnp.float32)
    return pl.pallas_call(
        own_kernel,
        compiler_params=LIMIT,
        in_specs=[SMEM, SMEM] + [VMEM] * 6,
        out_specs=(VMEM,) * 3,
        out_shape=(rows, rows, rows),
        scratch_shapes=[pltpu.VMEM((108, 512), jnp.float32)],
    )(where, fixes, *map(in_vmem, (totals, mine, theirs)), *states)


def assemble(c, mine, theirs, piece, weights):
    def kernel(c_ref, mine_ref, theirs_ref, *refs):
        out_ref = refs[-1]
        first = c_ref[0] == 0
        for half in range(2):
            for x, y in ((x, y) for x in range(2) for y in (half, 2 + half)):
                for z in range(8):
                    part = pl.ds(z * PART, PART)
                    own, other = mine_ref[8 * piece + 4 * x + y, part, :], theirs_ref[4 * x + y, part, :]
                    rows = pl.ds(864 * x + 108 * z + STARTS[half], PART)
                    for c in range(2):
                        cols = pl.ds((2 * c + y // 2) * 128, 128)
                        out_ref[rows, cols] = jnp.where(first == (c == 0), own, other)

    return pl.pallas_call(
        kernel,
        compiler_params=LIMIT,
        grid_spec=pltpu.PrefetchScalarGridSpec(
            num_scalar_prefetch=1,
            grid=(1,),
            in_specs=[VMEM, VMEM] + [ANY] * len(weights),
            out_specs=pl.BlockSpec((1728, 512), lambda i, c: (piece, 0)),
        ),
        out_shape=jax.ShapeDtypeStruct((3456, 512), jnp.bfloat16),
        input_output_aliases={3: 0} if weights else {},
    )(c, in_vmem(mine), in_vmem(theirs), *weights)


def shards(grads, master, moment_one, moment_two, step_count):
    y, c, z = (lax.axis_index(axis) for axis in ("y", "c", "z"))
    where = jnp.stack([y, c, z]).astype(jnp.int32)
    side = where[1:2]
    states = (master, moment_one, moment_two)
    steps = step_count[0].astype(jnp.float32)
    first_fix = 1.0 - jnp.power(jnp.float32(0.9), steps)
    second_fix = 1.0 - jnp.power(jnp.float32(0.999), steps)
    fixes = jnp.stack([first_fix, second_fix])
    local = grads[0, 0]
    theirs = [swapped(code_half(side, local, k), "c") for k in range(2)]
    coded = ()
    for k in range(2):
        coded = (code_sums(side, local, theirs[k], k, coded),)
    coded = exchanged(coded[0].reshape(16, COLUMN + 8, 128), PLANE)
    state_columns = rotated(state_parts(where, states), "z")
    coded, state_columns, fixes = lax.optimization_barrier((coded, state_columns, fixes))
    part, sent = part_sum(where, exchanged(sum_coded(coded), "z"))
    column = exchanged(sent, "z")
    own = column_total(column, rotated(part, "y"))
    other = swapped(own, "c")
    totals = exchanged(chip_total(own, other), PLANE)
    mine = exchanged(new_weights(where, fixes, totals, column, state_columns), PLANE)
    new = own_step(where, fixes, totals, own, other, states)
    theirs = [swapped(mine[8 * k : 8 * k + 8], "c") for k in range(2)]
    weights = ()
    for k in range(2):
        weights = (assemble(side, mine, theirs[k], k, weights),)
    return (*new, *weights)


def solution(mesh):
    finer = Mesh(mesh.devices.reshape(4, 2, 4, 8), ("y", "c", "x", "z"))
    in_specs = (P(GRP, SHARD, None, None), P(SHARD, None), P(SHARD, None), P(SHARD, None), P())
    out_specs = (P(SHARD, None), P(SHARD, None), P(SHARD, None), P())
    return jax.shard_map(
        shards, mesh=finer, in_specs=in_specs, out_specs=out_specs, check_vma=False
    )
```
